32 devices in a mesh: row: 4 (over y, x), col: 8 (over z, core).
Axes of the slice: x: 2, y: 2, z: 4, core: 2. Of those that a mesh axis runs over, the one named last changes fastest.
Arguments:
- right_side: bfloat16 [4, 8, 8, 128, 256], P('row', 'col'), may hold values from -6 to 6
- diag_inverse: bfloat16 [4, 8, 8, 128, 128], P('row', 'col'), may hold values from -0.5 to 0.5
- panels: bfloat16 [7, 4, 400, 128, 128], P(None, 'row', 'col'), may hold values from -0.0546875 to 0.0546875
- tile_source: int32 [7, 4, 400], P(None, 'row', 'col'), may hold values from 0 to 3
- tile_target: int32 [7, 4, 400], P(None, 'row', 'col'), may hold values from 0 to 7
Outputs:
- solution: float32 [4, 8, 8, 128, 256], P('row', 'col')
The draws below stay inside these ranges and needn't reach their ends.
All inputs are finite; a program needn't handle non-finite values.
Results may differ from the reference program's by a relative error of at most 0.017.
Values may be sent and summed in bfloat16 or wider, within the bound.
No kernel may reach another device: no remote copies, remote signals or barrier semaphores. Data moves between devices by JAX's collectives and lax.ppermute only.
A program may use at most 128 MiB of HBM per device.

```python
import jax
import jax.numpy as jnp
from jax import lax

BLOCK = 128
SECTIONS = 8
TPD = 50
COLS = 256
N_ROW = 4
N_COL = 8


def plant(result, rng, least, high):
    place = [jax.random.randint(jax.random.fold_in(rng, axis), (), 0, length) for axis, length in enumerate(result.shape)]
    widest = result.shape.index(max(result.shape))
    beside = place[:widest] + [(place[widest] + 1) % result.shape[widest]] + place[widest + 1:]
    return result.at[tuple(place)].set(least).at[tuple(beside)].set(high)


def block_levels(key, extent, split, smallest, largest):
    loudness = 1.0
    for axis_at, parts in split:
        steps = jax.random.uniform(jax.random.fold_in(jax.random.fold_in(key, 6), axis_at), (parts,), jnp.float32, smallest / len(split), largest / len(split))
        loudness = loudness * jnp.repeat(jnp.exp(steps), extent[axis_at] // parts).reshape((-1,) + (1,) * (len(extent) - 1 - axis_at))
    return loudness


def scatter_about(own_key, extent, deviation, reach, pieces=(), kind=jnp.bfloat16):
    factor_of = block_levels(own_key, extent, pieces, -0.22, 0.18) if pieces else 1.0
    array = jax.random.normal(own_key, extent, jnp.float32) * deviation * factor_of
    return jnp.minimum(jnp.maximum(array, -reach), reach).astype(kind)


def setup_inputs(seed: int = 0) -> dict:
    seeds = jax.random.split(jax.random.key(seed), 6)
    right_side = scatter_about(seeds[0], (N_ROW, N_COL, SECTIONS, BLOCK, COLS), 1.0, 6.0, ((0, 4), (1, 8)))
    diag_inverse = scatter_about(seeds[1], (N_ROW, N_COL, SECTIONS, BLOCK, BLOCK), BLOCK ** -0.5, 0.5, ((0, 4), (1, 8)))
    panels = scatter_about(seeds[2], (SECTIONS - 1, N_ROW, N_COL * TPD, BLOCK, BLOCK), (2 * BLOCK * TPD) ** -0.5, 0.0546875, ((1, 4), (2, 8)))
    tile_source = plant(jax.random.randint(seeds[3], (SECTIONS - 1, N_ROW, N_COL * TPD), 0, N_ROW), jax.random.fold_in(seeds[3], 1), 0, N_ROW - 1).astype(jnp.int32)
    tile_target = plant(jax.random.randint(seeds[4], (SECTIONS - 1, N_ROW, N_COL * TPD), 0, N_COL), jax.random.fold_in(seeds[4], 1), 0, N_COL - 1).astype(jnp.int32)
    return dict(right_side=right_side, diag_inverse=diag_inverse, panels=panels, tile_source=tile_source, tile_target=tile_target)


def round_trip(values):
    low = lax.optimization_barrier(values.astype(jnp.bfloat16))
    return low.astype(jnp.float32)


def reference(right_side, diag_inverse, panels, tile_source, tile_target):
    solved = []
    incoming = jnp.zeros((N_ROW, N_COL, BLOCK, COLS), jnp.float32)
    for section in range(SECTIONS):
        current = right_side[:, :, section].astype(jnp.float32)
        if section > 0:
            current = current - incoming
        current = round_trip(current)
        block = jnp.einsum("ijab,ijbc->ijac", diag_inverse[:, :, section].astype(jnp.float32), current,
                           precision=lax.Precision.HIGHEST)
        solved.append(block)
        if section + 1 < SECTIONS:
            segment = round_trip(block)

            def row_update(items):
                panel_row, source_row, target_row = items
                column_of = (jnp.arange(N_COL * TPD, dtype=jnp.int32) // TPD).astype(jnp.int32)
                picked = segment[source_row, column_of]
                prods = jnp.einsum("qab,qbc->qac", panel_row.astype(jnp.float32), picked,
                                   precision=lax.Precision.HIGHEST)
                prods = prods.reshape(N_COL, TPD, BLOCK * COLS)
                targets = target_row.reshape(N_COL, TPD)
                onehot = (targets[:, None, :] == jnp.arange(N_COL, dtype=jnp.int32)[None, :, None]).astype(jnp.float32)
                shard_sums = jnp.einsum("jtq,jqe->jte", onehot, prods, precision=lax.Precision.HIGHEST)
                shard_sums = round_trip(shard_sums)
                return jnp.sum(shard_sums, axis=0).reshape(N_COL, BLOCK, COLS)

            incoming = lax.map(row_update, (panels[section], tile_source[section], tile_target[section]))
    return jnp.stack(solved, axis=2)
```

```python
import functools

import jax
import jax.numpy as jnp
from jax import lax
from jax.experimental import pallas as pl
from jax.experimental.pallas import tpu as pltpu
from jax.sharding import PartitionSpec as P


def is_power(n):
    return n & (n - 1) == 0


def partner_of(index, step, count):
    return index ^ step if is_power(count) else (index + step) % count


def step_from(index, peer, count):
    return index ^ peer if is_power(count) else (index - peer) % count


def local_update(segment, panel, source, target):
    columns = lax.axis_size("col")
    picked = jnp.take(segment, source, axis=0)
    prods = jnp.einsum("qab,qbc->qac", panel, picked, preferred_element_type=jnp.float32)
    onehot = (target[None, :] == jnp.arange(columns, dtype=jnp.int32)[:, None]).astype(jnp.float32)
    sums = jnp.dot(onehot, prods.reshape(prods.shape[0], -1), precision=lax.Precision.HIGHEST)
    return sums.reshape(columns, prods.shape[1], prods.shape[2]).astype(jnp.bfloat16)


def advance_whole(block, panel, source, target):
    segment = lax.all_gather(block.astype(jnp.bfloat16)[None], "row", axis=0, tiled=True)
    partial_value = local_update(segment, panel, source, target)
    return lax.psum_scatter(partial_value, "col", scatter_dimension=0, tiled=True).astype(
        jnp.float32
    )[0]


def local_sparse(right_side, diag_inverse, panels, tile_source, tile_target):
    sections = right_side.shape[2]
    incoming = None
    solved = []
    for section in range(sections):
        current = right_side[0, 0, section].astype(jnp.float32)
        if section > 0:
            current = current - incoming
        block = jnp.dot(
            diag_inverse[0, 0, section],
            current.astype(jnp.bfloat16),
            preferred_element_type=jnp.float32,
        )
        if section + 1 < sections:
            incoming = advance_whole(
                block, panels[section, 0], tile_source[section, 0], tile_target[section, 0]
            )
        solved.append(block)
    return jnp.stack(solved, axis=0)[None, None]


def build_kernel(slot_ref, panel_ref, out_ref, acc_ref):
    acc_ref[...] = jnp.zeros_like(acc_ref)

    def add(q, carry):
        slot = slot_ref[q]
        acc_ref[slot] += panel_ref[0, 0, q].astype(jnp.float32)
        return carry

    lax.fori_loop(0, panel_ref.shape[2], add, 0)
    out_ref[...] = acc_ref[...].astype(out_ref.dtype)


def build_operator(level, slots, panels, count):
    tiles, rows, cols = panels.shape[2:]
    return pl.pallas_call(
        build_kernel,
        grid=(1,),
        out_shape=jax.ShapeDtypeStruct((count, rows, cols), panels.dtype),
        in_specs=[
            pl.BlockSpec(memory_space=pltpu.SMEM),
            pl.BlockSpec((1, 1, tiles, rows, cols), lambda i: (level, 0, 0, 0, 0)),
        ],
        out_specs=pl.BlockSpec((count, rows, cols), lambda i: (0, 0, 0)),
        scratch_shapes=[pltpu.VMEM((count, rows, cols), jnp.float32)],
        cost_estimate=pl.CostEstimate(
            flops=2_000_000_000,
            bytes_accessed=(tiles + count) * rows * cols * 2,
            transcendentals=0,
        ),
        name=f"build_{level}",
    )(slots, panels)


def local_dense(right_side, diag_inverse, panels, tile_source, tile_target):
    rows, columns = lax.axis_size("row"), lax.axis_size("col")
    chips = columns // 2
    sections, size, width = right_side.shape[2:]
    half = width // 2
    row, col = lax.axis_index("row"), lax.axis_index("col")
    chip, core = col // 2, col % 2
    swap_pairs = [(c, c ^ 1) for c in range(columns)]
    row_pairs = [[(r, partner_of(r, k, rows)) for r in range(rows)] for k in range(rows)]
    col_pairs = [
        [(c, 2 * partner_of(c // 2, k, chips) + c % 2) for c in range(columns)] for k in range(chips)
    ]

    source_slot = step_from(row, tile_source[:, 0], rows)
    target = tile_target[:, 0]
    target_slot = step_from(target // 2, chip, chips) * 2 + target % 2
    slots = source_slot * columns + target_slot

    mine = right_side[0, 0]
    low, high = mine[:, :, :half], mine[:, :, half:]
    first = core == 0
    kept = jnp.where(first, low, high)
    given = jnp.where(first, high, low)
    swapped = lax.ppermute(jnp.concatenate([given, diag_inverse[0, 0]], axis=-1), "col", swap_pairs)
    rights = jnp.stack([kept, swapped[:, :, :half]], axis=1)
    inverses = jnp.stack([diag_inverse[0, 0], swapped[:, :, half:]], axis=1)

    operators = []
    for section in range(sections - 1):
        own = build_operator(section, slots[section], panels, rows * columns)
        other = lax.ppermute(own, "col", swap_pairs)
        shape = (rows, columns * size, size)
        operators.append(jnp.concatenate([own.reshape(shape), other.reshape(shape)], axis=-1))

    solved_own, solved_other = [], []
    incoming = None
    for section in range(sections):
        current = rights[section].astype(jnp.float32)
        if section > 0:
            current = current - incoming
        block = jnp.einsum(
            "nab,nbc->nac",
            inverses[section],
            current.astype(jnp.bfloat16),
            preferred_element_type=jnp.float32,
        )
        solved_own.append(block[0])
        solved_other.append(lax.ppermute(block[1], "col", swap_pairs))
        if section + 1 < sections:
            segment = block.astype(jnp.bfloat16).reshape(2 * size, half)
            operator = operators[section]
            total = None
            heard = [segment] + [lax.ppermute(segment, "row", row_pairs[k]) for k in range(1, rows)]
            for k in range(rows):
                product = jnp.dot(operator[k], heard[k], preferred_element_type=jnp.float32)
                total = product if total is None else total + product
            partial = total.reshape(chips, 2, size, half)
            sums = partial[0]
            for k in range(1, chips):
                sums = sums + lax.ppermute(
                    partial[k].astype(jnp.bfloat16), "col", col_pairs[k]
                ).astype(jnp.float32)
            incoming = jnp.where(first, sums, sums[::-1])
    own, other = jnp.stack(solved_own), jnp.stack(solved_other)
    left = jnp.where(first, own, other)
    right = jnp.where(first, other, own)
    return jnp.concatenate([left, right], axis=-1)[None, None]


def solution(mesh):
    rows, columns = mesh.shape["row"], mesh.shape["col"]

    def local(right_side, diag_inverse, panels, tile_source, tile_target):
        dense = columns % 2 == 0 and rows * columns <= 2 * panels.shape[2]
        plan = local_dense if dense else local_sparse
        return plan(right_side, diag_inverse, panels, tile_source, tile_target)

    return jax.shard_map(
        local,
        mesh=mesh,
        in_specs=(
            P("row", "col", None, None, None),
            P("row", "col", None, None, None),
            P(None, "row", "col", None, None),
            P(None, "row", "col"),
            P(None, "row", "col"),
        ),
        out_specs=P("row", "col", None, None, None),
        check_vma=False,
    )
```

```python
import functools

import jax
import jax.numpy as jnp
from jax import lax
from jax.experimental import pallas as pl
from jax.experimental.pallas import tpu as pltpu
from jax.sharding import PartitionSpec as P


ROW_ORDER = (3, 1, 2)
COL_ORDER = (3, 2, 1)


def is_power(n):
    return n & (n - 1) == 0


def partner_of(index, step, count):
    return index ^ step if is_power(count) else (index + step) % count


def step_from(index, peer, count):
    return index ^ peer if is_power(count) else (index - peer) % count


def local_update(segment, panel, source, target):
    columns = lax.axis_size("col")
    picked = jnp.take(segment, source, axis=0)
    prods = jnp.einsum("qab,qbc->qac", panel, picked, preferred_element_type=jnp.float32)
    onehot = (target[None, :] == jnp.arange(columns, dtype=jnp.int32)[:, None]).astype(jnp.float32)
    sums = jnp.dot(onehot, prods.reshape(prods.shape[0], -1), precision=lax.Precision.HIGHEST)
    return sums.reshape(columns, prods.shape[1], prods.shape[2]).astype(jnp.bfloat16)


def advance_whole(block, panel, source, target):
    segment = lax.all_gather(block.astype(jnp.bfloat16)[None], "row", axis=0, tiled=True)
    partial_value = local_update(segment, panel, source, target)
    return lax.psum_scatter(partial_value, "col", scatter_dimension=0, tiled=True).astype(
        jnp.float32
    )[0]


def local_sparse(right_side, diag_inverse, panels, tile_source, tile_target):
    sections = right_side.shape[2]
    incoming = None
    solved = []
    for section in range(sections):
        current = right_side[0, 0, section].astype(jnp.float32)
        if section > 0:
            current = current - incoming
        block = jnp.dot(
            diag_inverse[0, 0, section],
            current.astype(jnp.bfloat16),
            preferred_element_type=jnp.float32,
        )
        if section + 1 < sections:
            incoming = advance_whole(
                block, panels[section, 0], tile_source[section, 0], tile_target[section, 0]
            )
        solved.append(block)
    return jnp.stack(solved, axis=0)[None, None]


def build_kernel(level, rows, columns, source_ref, target_ref, panel_ref, *refs):
    *out_refs, acc_ref = refs
    row, chip = lax.axis_index("row"), lax.axis_index("col") // 2
    acc_ref[...] = jnp.zeros_like(acc_ref)
    lead = (0,) * (len(panel_ref.shape) - 3)
    tiles = panel_ref.shape[len(lead)]

    def add(q, carry):
        target = target_ref[level, 0, q]
        step = step_from(row, source_ref[level, 0, q], rows)
        slot = step * columns + step_from(target // 2, chip, columns // 2) * 2 + target % 2
        acc_ref[slot] += panel_ref[(*lead, q)].astype(jnp.float32)
        return carry

    lax.fori_loop(0, tiles, add, 0, unroll=5 if tiles % 5 == 0 else 1)
    count = acc_ref.shape[0] // len(out_refs)
    for n, out_ref in enumerate(out_refs):
        out_ref[...] = acc_ref[pl.ds(n * count, count)].astype(out_ref.dtype)


def build_operator(level, sources, targets, panels, rows, columns, split):
    tiles, size, depth = panels.shape[-3:]
    pieces = rows if split else 1
    count = rows * columns // pieces
    lead = len(panels.shape) - 3
    index = (level, 0) if lead else ()
    out = pl.pallas_call(
        functools.partial(build_kernel, level, rows, columns),
        grid=(1,),
        out_shape=[jax.ShapeDtypeStruct((count, size, depth), panels.dtype)] * pieces,
        in_specs=[
            pl.BlockSpec(memory_space=pltpu.SMEM),
            pl.BlockSpec(memory_space=pltpu.SMEM),
            pl.BlockSpec((1,) * lead + panels.shape[-3:], lambda i: (*index, 0, 0, 0)),
        ],
        out_specs=[pl.BlockSpec((count, size, depth), lambda i: (0, 0, 0))] * pieces,
        scratch_shapes=[pltpu.VMEM((rows * columns, size, depth), jnp.float32)],
        compiler_params=pltpu.CompilerParams(
            vmem_limit_bytes=(4 * tiles + 8 * rows * columns) * size * depth + (2 << 20)
        ),
        cost_estimate=pl.CostEstimate(
            flops=2_000_000_000,
            bytes_accessed=(tiles + rows * columns) * size * depth * 2,
            transcendentals=0,
        ),
    )(sources, targets, panels)
    shape = (columns * size, depth)
    return [piece.reshape(shape) for piece in out] if split else out[0].reshape(rows, *shape)


def matmul(left, right):
    return jnp.dot(left, right, preferred_element_type=jnp.float32)


def local_dense(right_side, diag_inverse, panels, tile_source, tile_target):
    rows, columns = lax.axis_size("row"), lax.axis_size("col")
    chips = columns // 2
    sections, size, width = right_side.shape[2:]
    half = width // 2
    core = lax.axis_index("col") % 2
    swap_pairs = [(c, c ^ 1) for c in range(columns)]
    row_pairs = [[(r, partner_of(r, k, rows)) for r in range(rows)] for k in range(rows)]
    col_pairs = [
        [(c, 2 * partner_of(c // 2, k, chips) + c % 2) for c in range(columns)] for k in range(chips)
    ]

    def kept_half(values):
        return jnp.where(core == 0, values[..., :half], values[..., half:])

    def given_half(values):
        return jnp.where(core == 0, values[..., half:], values[..., :half])

    def built(section, split=False):
        tiles = panels[section, 0] if split else panels
        return build_operator(section, tile_source, tile_target, tiles, rows, columns, split)

    def traded(own):
        other = lax.ppermute(own, "col", swap_pairs)
        return jnp.concatenate([own, other], axis=-1)

    def gathered(segment):
        heard = {0: segment}
        for k in row_order(rows):
            heard[k] = lax.ppermute(segment, "row", row_pairs[k])
        return heard

    def applied(operator, heard):
        *early, last = [0] + row_order(rows)
        products = []
        for k in early:
            products.append(lax.optimization_barrier(matmul(operator[k], heard[k])))
        return sum(products[1:], products[0]) + matmul(operator[last], heard[last])

    def reduced(total):
        total = total.reshape(chips, 2 * size, half)
        sent = total.astype(jnp.bfloat16)
        arrived = []
        for k in col_order(chips):
            arrived.append(lax.ppermute(sent[k], "col", col_pairs[k]))
        sums = total[0]
        for value in arrived:
            sums = sums + value.astype(jnp.float32)
        sums = sums.reshape(2, size, half)
        return jnp.where(core == 0, sums, sums[::-1])

    def placed(answer, section, values):
        return lax.dynamic_update_slice(answer, values[None, None, None], (0, 0, section, 0, 0))

    block = matmul(diag_inverse[0, 0, 0], right_side[0, 0, 0])
    heard = gathered(block.astype(jnp.bfloat16))
    own = built(0, split=True)
    other_right = lax.ppermute(right_side, "col", swap_pairs)
    other_inverse = lax.ppermute(diag_inverse, "col", swap_pairs)
    total = applied(own, heard)
    share = lax.ppermute(given_half(total).astype(jnp.bfloat16), "col", swap_pairs)
    total = kept_half(total) + share.astype(jnp.float32)
    incoming = reduced(total)
    operator = traded(built(1)) if sections > 2 else None
    answer = placed(jnp.zeros((1, 1, sections, size, width), jnp.float32), 0, block)
    rights = kept_half(jnp.stack([right_side[0, 0], other_right[0, 0]], axis=1))
    inverses = jnp.stack([diag_inverse[0, 0], other_inverse[0, 0]], axis=1)
    rights, inverses = lax.optimization_barrier((rights, inverses))

    for section in range(1, sections):
        current = rights[section].astype(jnp.float32) - incoming
        block = jnp.einsum(
            "nab,nbc->nac",
            inverses[section],
            current.astype(jnp.bfloat16),
            preferred_element_type=jnp.float32,
        )
        other = lax.ppermute(block[1], "col", swap_pairs)
        if section + 1 < sections:
            heard = gathered(block.astype(jnp.bfloat16).reshape(2 * size, half))
            incoming = reduced(applied(operator, heard))
            if section + 2 < sections:
                operator = traded(built(section + 1))
        left = jnp.where(core == 0, block[0], other)
        right = jnp.where(core == 0, other, block[0])
        answer = placed(answer, section, jnp.concatenate([left, right], axis=-1))
    return answer


def row_order(rows):
    return [k for k in ROW_ORDER if k < rows] + [k for k in range(1, rows) if k not in ROW_ORDER]


def col_order(chips):
    return [k for k in COL_ORDER if k < chips] + [k for k in range(1, chips) if k not in COL_ORDER]


def solution(mesh):
    rows, columns = mesh.shape["row"], mesh.shape["col"]

    def local(right_side, diag_inverse, panels, tile_source, tile_target):
        dense = columns % 2 == 0 and rows * columns <= 2 * panels.shape[2]
        plan = local_dense if dense else local_sparse
        return plan(right_side, diag_inverse, panels, tile_source, tile_target)

    return jax.shard_map(
        local,
        mesh=mesh,
        in_specs=(
            P("row", "col", None, None, None),
            P("row", "col", None, None, None),
            P(None, "row", "col", None, None),
            P(None, "row", "col"),
            P(None, "row", "col"),
        ),
        out_specs=P("row", "col", None, None, None),
        check_vma=False,
    )
```

```python
import functools

import jax
import jax.numpy as jnp
from jax import lax
from jax.experimental import pallas as pl
from jax.experimental.pallas import tpu as pltpu
from jax.sharding import PartitionSpec as P


ROW_ORDER = (3, 1, 2)
COL_ORDER = (3, 2, 1)


def is_power(n):
    return n & (n - 1) == 0


def partner_of(index, step, count):
    return index ^ step if is_power(count) else (index + step) % count


def step_from(index, peer, count):
    return index ^ peer if is_power(count) else (index - peer) % count


def local_update(segment, panel, source, target):
    columns = lax.axis_size("col")
    picked = jnp.take(segment, source, axis=0)
    prods = jnp.einsum("qab,qbc->qac", panel, picked, preferred_element_type=jnp.float32)
    onehot = (target[None, :] == jnp.arange(columns, dtype=jnp.int32)[:, None]).astype(jnp.float32)
    sums = jnp.dot(onehot, prods.reshape(prods.shape[0], -1), precision=lax.Precision.HIGHEST)
    return sums.reshape(columns, prods.shape[1], prods.shape[2]).astype(jnp.bfloat16)


def advance_whole(block, panel, source, target):
    segment = lax.all_gather(block.astype(jnp.bfloat16)[None], "row", axis=0, tiled=True)
    partial_value = local_update(segment, panel, source, target)
    return lax.psum_scatter(partial_value, "col", scatter_dimension=0, tiled=True).astype(
        jnp.float32
    )[0]


def local_sparse(right_side, diag_inverse, panels, tile_source, tile_target):
    sections = right_side.shape[2]
    incoming = None
    solved = []
    for section in range(sections):
        current = right_side[0, 0, section].astype(jnp.float32)
        if section > 0:
            current = current - incoming
        block = jnp.dot(
            diag_inverse[0, 0, section],
            current.astype(jnp.bfloat16),
            preferred_element_type=jnp.float32,
        )
        if section + 1 < sections:
            incoming = advance_whole(
                block, panels[section, 0], tile_source[section, 0], tile_target[section, 0]
            )
        solved.append(block)
    return jnp.stack(solved, axis=0)[None, None]


def build_kernel(level, rows, columns, source_ref, target_ref, panel_ref, *refs):
    *out_refs, acc_ref = refs
    row, chip = lax.axis_index("row"), lax.axis_index("col") // 2
    acc_ref[...] = jnp.zeros_like(acc_ref)
    lead = (0,) * (len(panel_ref.shape) - 3)
    tiles = panel_ref.shape[len(lead)]

    def add(q, carry):
        target = target_ref[level, 0, q]
        step = step_from(row, source_ref[level, 0, q], rows)
        slot = step * columns + step_from(target // 2, chip, columns // 2) * 2 + target % 2
        acc_ref[slot] += panel_ref[(*lead, q)].astype(jnp.float32)
        return carry

    lax.fori_loop(0, tiles, add, 0, unroll=5 if tiles % 5 == 0 else 1)
    count = acc_ref.shape[0] // len(out_refs)
    for n, out_ref in enumerate(out_refs):
        out_ref[...] = acc_ref[pl.ds(n * count, count)].astype(out_ref.dtype)


def build_operator(level, sources, targets, panels, rows, columns, split):
    tiles, size, depth = panels.shape[-3:]
    pieces = rows if split else 1
    count = rows * columns // pieces
    lead = len(panels.shape) - 3
    index = (level, 0) if lead else ()
    out = pl.pallas_call(
        functools.partial(build_kernel, level, rows, columns),
        grid=(1,),
        out_shape=[jax.ShapeDtypeStruct((count, size, depth), panels.dtype)] * pieces,
        in_specs=[
            pl.BlockSpec(memory_space=pltpu.SMEM),
            pl.BlockSpec(memory_space=pltpu.SMEM),
            pl.BlockSpec((1,) * lead + panels.shape[-3:], lambda i: (*index, 0, 0, 0)),
        ],
        out_specs=[pl.BlockSpec((count, size, depth), lambda i: (0, 0, 0))] * pieces,
        scratch_shapes=[pltpu.VMEM((rows * columns, size, depth), jnp.float32)],
        compiler_params=pltpu.CompilerParams(
            vmem_limit_bytes=(4 * tiles + 8 * rows * columns) * size * depth + (2 << 20)
        ),
        cost_estimate=pl.CostEstimate(
            flops=2_000_000_000,
            bytes_accessed=(tiles + rows * columns) * size * depth * 2,
            transcendentals=0,
        ),
    )(sources, targets, panels)
    shape = (columns * size, depth)
    return [piece.reshape(shape) for piece in out] if split else out[0].reshape(rows, *shape)


def matmul(left, right):
    return jnp.dot(left, right, preferred_element_type=jnp.float32)


def local_dense(right_side, diag_inverse, panels, tile_source, tile_target):
    rows, columns = lax.axis_size("row"), lax.axis_size("col")
    chips = columns // 2
    sections, size, width = right_side.shape[2:]
    half = width // 2
    core = lax.axis_index("col") % 2
    swap_pairs = [(c, c ^ 1) for c in range(columns)]
    row_pairs = [[(r, partner_of(r, k, rows)) for r in range(rows)] for k in range(rows)]
    col_pairs = [
        [(c, 2 * partner_of(c // 2, k, chips) + c % 2) for c in range(columns)] for k in range(chips)
    ]

    def kept_half(values):
        return jnp.where(core == 0, values[..., :half], values[..., half:])

    def given_half(values):
        return jnp.where(core == 0, values[..., half:], values[..., :half])

    def built(section, split=False):
        tiles = panels[section, 0] if split else panels
        return build_operator(section, tile_source, tile_target, tiles, rows, columns, split)

    def traded(own):
        other = lax.ppermute(own, "col", swap_pairs)
        return jnp.concatenate([own, other], axis=-1)

    def gathered(segment):
        heard = {0: segment}
        for k in row_order(rows):
            heard[k] = lax.ppermute(segment, "row", row_pairs[k])
        return heard

    def applied(operator, heard):
        *early, last = [0] + row_order(rows)
        products = []
        for k in early:
            products.append(lax.optimization_barrier(matmul(operator[k], heard[k])))
        return sum(products[1:], products[0]) + matmul(operator[last], heard[last])

    def reduced(total):
        total = total.reshape(chips, 2 * size, half)
        sent = total.astype(jnp.bfloat16)
        arrived = []
        for k in col_order(chips):
            arrived.append(lax.ppermute(sent[k], "col", col_pairs[k]))
        sums = total[0]
        for value in arrived:
            sums = sums + value.astype(jnp.float32)
        sums = sums.reshape(2, size, half)
        return jnp.where(core == 0, sums, sums[::-1])

    def placed(answer, section, values):
        return lax.dynamic_update_slice(answer, values[None, None, None], (0, 0, section, 0, 0))

    block = matmul(diag_inverse[0, 0, 0], right_side[0, 0, 0])
    heard = gathered(block.astype(jnp.bfloat16))
    own = built(0, split=True)
    other_right = lax.ppermute(right_side, "col", swap_pairs)
    other_inverse = lax.ppermute(diag_inverse, "col", swap_pairs)
    order = [0] + row_order(rows)
    total = None
    for pair in (order[n : n + 2] for n in range(0, rows, 2)):
        product = matmul(
            jnp.concatenate([own[k] for k in pair], axis=-1),
            jnp.concatenate([heard[k] for k in pair], axis=0),
        )
        total = product if total is None else lax.optimization_barrier(total) + product
    share = lax.ppermute(given_half(total).astype(jnp.bfloat16), "col", swap_pairs)
    total = kept_half(total) + share.astype(jnp.float32)
    incoming = reduced(total)
    operator = traded(built(1)) if sections > 2 else None
    answer = placed(jnp.zeros((1, 1, sections, size, width), jnp.float32), 0, block)
    rights = kept_half(jnp.stack([right_side[0, 0], other_right[0, 0]], axis=1))
    inverses = jnp.stack([diag_inverse[0, 0], other_inverse[0, 0]], axis=1)
    rights, inverses = lax.optimization_barrier((rights, inverses))

    pending = []
    for section in range(1, sections):
        current = rights[section].astype(jnp.float32) - incoming
        block = jnp.einsum(
            "nab,nbc->nac",
            inverses[section],
            current.astype(jnp.bfloat16),
            preferred_element_type=jnp.float32,
        )
        pending.append((section, block))
        if section + 2 == sections or section + 1 == sections:
            others = lax.ppermute(jnp.stack([b[1] for _, b in pending]), "col", swap_pairs)
        if section + 1 < sections:
            heard = gathered(block.astype(jnp.bfloat16).reshape(2 * size, half))
            incoming = reduced(applied(operator, heard))
            if section + 2 < sections:
                operator = traded(built(section + 1))
        if section + 2 >= sections:
            kept = jnp.stack([b[0] for _, b in pending])
            left = jnp.where(core == 0, kept, others)
            right = jnp.where(core == 0, others, kept)
            answer = lax.dynamic_update_slice(answer, jnp.concatenate([left, right], axis=-1)[None, None], (0, 0, pending[0][0], 0, 0))
            pending = []
    return answer


def row_order(rows):
    return [k for k in ROW_ORDER if k < rows] + [k for k in range(1, rows) if k not in ROW_ORDER]


def col_order(chips):
    return [k for k in COL_ORDER if k < chips] + [k for k in range(1, chips) if k not in COL_ORDER]


def solution(mesh):
    rows, columns = mesh.shape["row"], mesh.shape["col"]

    def local(right_side, diag_inverse, panels, tile_source, tile_target):
        dense = columns % 2 == 0 and rows * columns <= 2 * panels.shape[2]
        plan = local_dense if dense else local_sparse
        return plan(right_side, diag_inverse, panels, tile_source, tile_target)

    return jax.shard_map(
        local,
        mesh=mesh,
        in_specs=(
            P("row", "col", None, None, None),
            P("row", "col", None, None, None),
            P(None, "row", "col", None, None),
            P(None, "row", "col"),
            P(None, "row", "col"),
        ),
        out_specs=P("row", "col", None, None, None),
        check_vma=False,
    )
```

```python
import functools

import jax
import jax.numpy as jnp
from jax import lax
from jax.experimental import pallas as pl
from jax.experimental.pallas import tpu as pltpu
from jax.sharding import PartitionSpec as P


ROW_ORDER = (3, 1, 2)
COL_ORDER = (3, 2, 1)


def is_power(n):
    return n & (n - 1) == 0


def partner_of(index, step, count):
    return index ^ step if is_power(count) else (index + step) % count


def step_from(index, peer, count):
    return index ^ peer if is_power(count) else (index - peer) % count


def local_update(segment, panel, source, target):
    columns = lax.axis_size("col")
    picked = jnp.take(segment, source, axis=0)
    prods = jnp.einsum("qab,qbc->qac", panel, picked, preferred_element_type=jnp.float32)
    onehot = (target[None, :] == jnp.arange(columns, dtype=jnp.int32)[:, None]).astype(jnp.float32)
    sums = jnp.dot(onehot, prods.reshape(prods.shape[0], -1), precision=lax.Precision.HIGHEST)
    return sums.reshape(columns, prods.shape[1], prods.shape[2]).astype(jnp.bfloat16)


def advance_whole(block, panel, source, target):
    segment = lax.all_gather(block.astype(jnp.bfloat16)[None], "row", axis=0, tiled=True)
    partial_value = local_update(segment, panel, source, target)
    return lax.psum_scatter(partial_value, "col", scatter_dimension=0, tiled=True).astype(
        jnp.float32
    )[0]


def local_sparse(right_side, diag_inverse, panels, tile_source, tile_target):
    sections = right_side.shape[2]
    incoming = None
    solved = []
    for section in range(sections):
        current = right_side[0, 0, section].astype(jnp.float32)
        if section > 0:
            current = current - incoming
        block = jnp.dot(
            diag_inverse[0, 0, section],
            current.astype(jnp.bfloat16),
            preferred_element_type=jnp.float32,
        )
        if section + 1 < sections:
            incoming = advance_whole(
                block, panels[section, 0], tile_source[section, 0], tile_target[section, 0]
            )
        solved.append(block)
    return jnp.stack(solved, axis=0)[None, None]


def build_kernel(level, rows, columns, source_ref, target_ref, panel_ref, *refs):
    *out_refs, acc_ref = refs
    row, chip = lax.axis_index("row"), lax.axis_index("col") // 2
    acc_ref[...] = jnp.zeros_like(acc_ref)
    lead = (0,) * (len(panel_ref.shape) - 3)
    tiles = panel_ref.shape[len(lead)]

    def add(q, carry):
        target = target_ref[level, 0, q]
        step = step_from(row, source_ref[level, 0, q], rows)
        slot = step * columns + step_from(target // 2, chip, columns // 2) * 2 + target % 2
        acc_ref[slot] += panel_ref[(*lead, q)].astype(jnp.float32)
        return carry

    lax.fori_loop(0, tiles, add, 0, unroll=5 if tiles % 5 == 0 else 1)
    count = acc_ref.shape[0] // len(out_refs)
    for n, out_ref in enumerate(out_refs):
        out_ref[...] = acc_ref[pl.ds(n * count, count)].astype(out_ref.dtype)


def build_operator(level, sources, targets, panels, rows, columns, split):
    tiles, size, depth = panels.shape[-3:]
    pieces = rows if split else 1
    count = rows * columns // pieces
    lead = len(panels.shape) - 3
    index = (level, 0) if lead else ()
    out = pl.pallas_call(
        functools.partial(build_kernel, level, rows, columns),
        grid=(1,),
        out_shape=[jax.ShapeDtypeStruct((count, size, depth), panels.dtype)] * pieces,
        in_specs=[
            pl.BlockSpec(memory_space=pltpu.SMEM),
            pl.BlockSpec(memory_space=pltpu.SMEM),
            pl.BlockSpec((1,) * lead + panels.shape[-3:], lambda i: (*index, 0, 0, 0)),
        ],
        out_specs=[pl.BlockSpec((count, size, depth), lambda i: (0, 0, 0))] * pieces,
        scratch_shapes=[pltpu.VMEM((rows * columns, size, depth), jnp.float32)],
        compiler_params=pltpu.CompilerParams(
            vmem_limit_bytes=(4 * tiles + 8 * rows * columns) * size * depth + (2 << 20)
        ),
        cost_estimate=pl.CostEstimate(
            flops=2_000_000_000,
            bytes_accessed=(tiles + rows * columns) * size * depth * 2,
            transcendentals=0,
        ),
    )(sources, targets, panels)
    shape = (columns * size, depth)
    return [piece.reshape(shape) for piece in out] if split else out[0].reshape(rows, *shape)


def matmul(left, right):
    return jnp.dot(left, right, preferred_element_type=jnp.float32)


def local_dense(right_side, diag_inverse, panels, tile_source, tile_target):
    rows, columns = lax.axis_size("row"), lax.axis_size("col")
    chips = columns // 2
    sections, size, width = right_side.shape[2:]
    half = width // 2
    core = lax.axis_index("col") % 2
    swap_pairs = [(c, c ^ 1) for c in range(columns)]
    row_pairs = [[(r, partner_of(r, k, rows)) for r in range(rows)] for k in range(rows)]
    col_pairs = [
        [(c, 2 * partner_of(c // 2, k, chips) + c % 2) for c in range(columns)] for k in range(chips)
    ]

    def kept_half(values):
        return jnp.where(core == 0, values[..., :half], values[..., half:])

    def given_half(values):
        return jnp.where(core == 0, values[..., half:], values[..., :half])

    def built(section, split=False):
        tiles = panels[section, 0] if split else panels
        return build_operator(section, tile_source, tile_target, tiles, rows, columns, split)

    def traded(own):
        other = lax.ppermute(own, "col", swap_pairs)
        return jnp.concatenate([own, other], axis=-1)

    def gathered(segment):
        heard = {0: segment}
        for k in row_order(rows):
            heard[k] = lax.ppermute(segment, "row", row_pairs[k])
        return heard

    def applied(operator, heard):
        *early, last = [0] + row_order(rows)
        products = []
        for k in early:
            products.append(lax.optimization_barrier(matmul(operator[k], heard[k])))
        return sum(products[1:], products[0]) + matmul(operator[last], heard[last])

    def reduced(total):
        total = total.reshape(chips, 2 * size, half)
        sent = total.astype(jnp.bfloat16)
        arrived = []
        for k in col_order(chips):
            arrived.append(lax.ppermute(sent[k], "col", col_pairs[k]))
        sums = jnp.zeros((2, size, half), jnp.float32)
        for value in [total[0], *arrived]:
            value = value.reshape(2, size, half)
            sums = sums + jnp.where(core == 0, value, value[::-1]).astype(jnp.float32)
        return sums

    def placed(answer, section, values):
        return lax.dynamic_update_slice(answer, values[None, None, None], (0, 0, section, 0, 0))

    block = matmul(diag_inverse[0, 0, 0], right_side[0, 0, 0])
    heard = gathered(block.astype(jnp.bfloat16))
    own = built(0, split=True)
    other_right = lax.ppermute(right_side, "col", swap_pairs)
    other_inverse = lax.ppermute(diag_inverse, "col", swap_pairs)
    order = [0] + row_order(rows)
    total = None
    for pair in (order[n : n + 2] for n in range(0, rows, 2)):
        product = matmul(
            jnp.concatenate([own[k] for k in pair], axis=-1),
            jnp.concatenate([heard[k] for k in pair], axis=0),
        )
        total = product if total is None else lax.optimization_barrier(total) + product
    share = lax.ppermute(given_half(total).astype(jnp.bfloat16), "col", swap_pairs)
    total = kept_half(total) + share.astype(jnp.float32)
    incoming = reduced(total)
    operator = traded(built(1)) if sections > 2 else None
    answer = placed(jnp.zeros((1, 1, sections, size, width), jnp.float32), 0, block)
    rights = kept_half(jnp.stack([right_side[0, 0], other_right[0, 0]], axis=1))
    inverses = jnp.stack([diag_inverse[0, 0], other_inverse[0, 0]], axis=1)
    rights, inverses = lax.optimization_barrier((rights, inverses))

    pending = []
    for section in range(1, sections):
        current = rights[section].astype(jnp.float32) - incoming
        block = jnp.einsum(
            "nab,nbc->nac",
            inverses[section],
            current.astype(jnp.bfloat16),
            preferred_element_type=jnp.float32,
        )
        pending.append((section, block))
        if section + 2 == sections or section + 1 == sections:
            others = lax.ppermute(jnp.stack([b[1] for _, b in pending]), "col", swap_pairs)
        if section + 1 < sections:
            heard = gathered(block.astype(jnp.bfloat16).reshape(2 * size, half))
            incoming = reduced(applied(operator, heard))
            if section + 2 < sections:
                operator = traded(built(section + 1))
        if section + 2 >= sections:
            kept = jnp.stack([b[0] for _, b in pending])
            left = jnp.where(core == 0, kept, others)
            right = jnp.where(core == 0, others, kept)
            answer = lax.dynamic_update_slice(answer, jnp.concatenate([left, right], axis=-1)[None, None], (0, 0, pending[0][0], 0, 0))
            pending = []
    return answer


def row_order(rows):
    return [k for k in ROW_ORDER if k < rows] + [k for k in range(1, rows) if k not in ROW_ORDER]


def col_order(chips):
    return [k for k in COL_ORDER if k < chips] + [k for k in range(1, chips) if k not in COL_ORDER]


def solution(mesh):
    rows, columns = mesh.shape["row"], mesh.shape["col"]

    def local(right_side, diag_inverse, panels, tile_source, tile_target):
        dense = columns % 2 == 0 and rows * columns <= 2 * panels.shape[2]
        plan = local_dense if dense else local_sparse
        return plan(right_side, diag_inverse, panels, tile_source, tile_target)

    return jax.shard_map(
        local,
        mesh=mesh,
        in_specs=(
            P("row", "col", None, None, None),
            P("row", "col", None, None, None),
            P(None, "row", "col", None, None),
            P(None, "row", "col"),
            P(None, "row", "col"),
        ),
        out_specs=P("row", "col", None, None, None),
        check_vma=False,
    )
```
